32 devices in a mesh: tm: 8 (over y, x, core), series: 4 (over z).
Axes of the slice: x: 2, y: 2, z: 4, core: 2. Of those that a mesh axis runs over, the one named last changes fastest.
Arguments:
- tokens: bfloat16 [8, 4096, 1024], P('series', 'tm'), may hold values from -6 to 6
- gate_proj: bfloat16 [1024, 2048], replicated, may hold values from -0.1875 to 0.1875
- input_proj: bfloat16 [1024, 2304], replicated, may hold values from -0.1875 to 0.1875
- step_proj: bfloat16 [1024, 32], replicated, may hold values from -0.1875 to 0.1875
- conv_kernel: float32 [4, 2304], replicated, may hold values from -3 to 3
- conv_bias: float32 [2304], replicated, may hold values from -0.5 to 0.5
- step_bias: float32 [32], replicated, may hold values from -1 to 1
- decay_rate: float32 [32], replicated, may hold values from 0.00012207031 to 0.1
- skip_gain: float32 [32], replicated, may hold values from 0.5 to 1.5
- norm_gain: float32 [2048], replicated, may hold values from 0.1 to 1.9
- out_proj: bfloat16 [2048, 1024], replicated, may hold values from -0.125 to 0.125
- lengths: int32 [8], P('series'), may hold values from 256 to 4096, as said below
- slot_series: int32 [8], P('series'), may hold values from 0 to 7, each once
Outputs:
- mixed: bfloat16 [8, 4096, 1024], P('series', 'tm')
The draws below stay inside these ranges and needn't reach their ends.
Inputs may be any that keep to these rules, and one draw needn't show every extreme that they name: `lengths`: multiples of 256; some series has the full 4096. `slot_series`: each series number appears once.
All inputs are finite; a program needn't handle non-finite values.
Results may differ from the reference program's by a relative error of at most 0.0054.
Values may be sent and summed in bfloat16 or wider, within the bound.
A program may use at most 128 MiB of HBM per device.

```python
import math
import jax
import jax.numpy as jnp
from jax import lax

D = 1024
DI = 2048
H = 32
P_SIZE = 64
N = 128
KERNEL = 4
BLOCK = 256
SERIES = 8
STEPS = 4096


def draw_lengths(key, part):
    blocks_total = STEPS // BLOCK
    counts = jax.random.randint(jax.random.fold_in(key, 11), (SERIES,), 1, blocks_total + 1)
    full_one = jax.random.randint(jax.random.fold_in(key, 12), (), 0, SERIES)
    counts = jnp.where(jnp.arange(SERIES) == full_one, blocks_total, counts)
    return (counts * BLOCK).astype(jnp.int32)


def block_levels(rng, extent, cuts, least, largest):
    level, own = 1.0, jax.random.fold_in(rng, 6)
    for dim, shards_of in cuts:
        steps = jnp.exp(jax.random.uniform(jax.random.fold_in(own, dim), (shards_of,), jnp.float32, least / len(cuts), largest / len(cuts)))
        level = level * jnp.repeat(steps, extent[dim] // shards_of).reshape([-1 if axis == dim else 1 for axis in range(len(extent))])
    return level


def scatter_about(rng, shape, scale, reach, split=(), held_as=jnp.bfloat16):
    entries = scale * jax.random.normal(rng, shape, jnp.float32)
    if split:
        entries = entries * block_levels(rng, shape, split, -0.22, 0.18)
    return jnp.clip(entries, -reach, reach).astype(held_as)


def setup_inputs(seed: int = 0) -> dict:
    splits = jax.random.split(jax.random.key(seed), 14)
    return {
        "tokens": scatter_about(splits[0], (SERIES, STEPS, D), 1.0, 6.0, ((0, 4), (1, 8))),
        "gate_proj": scatter_about(splits[1], (D, DI), D ** -0.5, 0.1875),
        "input_proj": scatter_about(splits[2], (D, DI + 2 * N), D ** -0.5, 0.1875),
        "step_proj": scatter_about(splits[3], (D, H), D ** -0.5, 0.1875),
        "conv_kernel": scatter_about(splits[4], (KERNEL, DI + 2 * N), 0.5, 3.0, (), jnp.float32),
        "conv_bias": jnp.clip(jax.random.uniform(splits[5], (DI + 2 * N,), jnp.float32, -0.5, 0.5), -0.5, 0.5),
        "step_bias": jnp.clip(jax.random.uniform(splits[6], (H,), jnp.float32, -1.0, 1.0), -1.0, 1.0),
        "decay_rate": jnp.clip(jnp.exp(jax.random.uniform(splits[7], (H,), jnp.float32, math.log(0.00012207031), math.log(0.1))), 0.00012207031, 0.1),
        "skip_gain": jnp.clip(jax.random.uniform(splits[8], (H,), jnp.float32, 0.5, 1.5), 0.5, 1.5),
        "norm_gain": jnp.clip(1.0 + 0.18 * jax.random.normal(splits[9], (DI,), jnp.float32), 0.1, 1.9),
        "out_proj": scatter_about(splits[10], (DI, D), DI ** -0.5, 0.125),
        "lengths": draw_lengths(jax.random.fold_in(splits[13], 71), 0),
        "slot_series": jax.random.permutation(splits[12], SERIES).astype(jnp.int32),
    }


epsilon = 1e-05

def block_terms(inputs_x, inputs_b, inputs_c, step_sizes, decay_rate, skip_gain):
    width_q = inputs_x.shape[0]
    cumulative = jnp.cumsum(-step_sizes * decay_rate[None, :], axis=0)
    heads_cum = cumulative.T
    causal = jnp.tril(jnp.ones((width_q, width_q), dtype=bool))[None]
    segment = heads_cum[:, :, None] - heads_cum[:, None, :]
    decays = jnp.where(causal, jnp.exp(jnp.where(causal, segment, 0.0)), 0.0)
    scores = jnp.dot(inputs_c, inputs_b.T, preferred_element_type=jnp.float32)
    weights = (decays * scores[None] * step_sizes.T[:, None, :]).astype(jnp.bfloat16)
    intra = jnp.einsum('hts,shp->thp', weights.astype(jnp.float32), inputs_x.astype(jnp.float32))
    partial_out = intra + skip_gain[None, :, None] * inputs_x.astype(jnp.float32)
    end_weight = jnp.exp(cumulative[-1][None, :] - cumulative) * step_sizes
    weighted_x = (inputs_x.astype(jnp.float32) * end_weight[:, :, None]).astype(jnp.bfloat16)
    increment = jnp.einsum('shp,sn->hpn', weighted_x.astype(jnp.float32), inputs_b.astype(jnp.float32))
    return (partial_out, cumulative, increment)

def reference(tokens, gate_proj, input_proj, step_proj, conv_kernel, conv_bias, step_bias, decay_rate, skip_gain, norm_gain, out_proj, lengths, slot_series):
    series_lengths = lengths[slot_series]

    def one_series(pair):
        row_tokens, length_now = pair
        total_steps = row_tokens.shape[0]
        gate = jnp.dot(row_tokens, gate_proj, preferred_element_type=jnp.float32)
        mixed_raw = jnp.dot(row_tokens, input_proj, preferred_element_type=jnp.float32).astype(jnp.bfloat16)
        step_raw = jnp.dot(row_tokens, step_proj, preferred_element_type=jnp.float32)
        kernel_len = conv_kernel.shape[0]
        padded = jnp.concatenate([jnp.zeros((kernel_len - 1, mixed_raw.shape[1]), jnp.bfloat16), mixed_raw], axis=0)
        convolved = jnp.zeros(mixed_raw.shape, jnp.float32) + conv_bias[None, :]
        for offset in range(kernel_len):
            convolved = convolved + conv_kernel[offset][None, :] * padded[offset:offset + total_steps].astype(jnp.float32)
        activated = jax.nn.silu(convolved)
        block_count = total_steps // BLOCK
        inputs_x = activated[:, :DI].astype(jnp.bfloat16).reshape(block_count, BLOCK, H, P_SIZE)
        inputs_b = activated[:, DI:DI + N].astype(jnp.bfloat16).reshape(block_count, BLOCK, N)
        inputs_c = activated[:, DI + N:].astype(jnp.bfloat16).reshape(block_count, BLOCK, N)
        live = (jnp.arange(total_steps, dtype=jnp.int32) < length_now).astype(jnp.float32)
        step_sizes = (jax.nn.softplus(step_raw + step_bias[None, :]) * live[:, None]).reshape(block_count, BLOCK, H)

        def advance(state, pieces):
            block_x, block_b, block_c, block_dt = pieces
            partial_out, cumulative, increment = block_terms(block_x, block_b, block_c, block_dt, decay_rate, skip_gain)
            state_bf = state.astype(jnp.bfloat16)
            inter = jnp.einsum('tn,hpn->thp', block_c.astype(jnp.float32), state_bf.astype(jnp.float32))
            output = partial_out + jnp.exp(cumulative)[:, :, None] * inter
            state = jnp.exp(cumulative[-1])[:, None, None] * state + increment
            return (state, output)
        start_state = jnp.zeros((H, P_SIZE, N), jnp.float32)
        ignored, outputs = lax.scan(advance, start_state, (inputs_x, inputs_b, inputs_c, step_sizes))
        outputs = outputs.reshape(total_steps, DI)
        gated = outputs * jax.nn.silu(gate)
        scale = lax.rsqrt(lax.optimization_barrier(jnp.mean(gated * gated, axis=1, keepdims=True)) + epsilon)
        normed = (gated * scale * norm_gain[None, :]).astype(jnp.bfloat16)
        result = jnp.dot(normed, out_proj, preferred_element_type=jnp.float32) * live[:, None]
        return result.astype(jnp.bfloat16)
    return lax.map(one_series, (tokens, series_lengths))
```

```python
import functools

import jax
import jax.numpy as jnp
from jax import lax
from jax.experimental import pallas as pl
from jax.experimental.pallas import tpu as pltpu
from jax.sharding import PartitionSpec as P

BLOCK = 256
CHUNK = 256
LANES = 128
TAIL = 16
EPSILON = 1e-05
F32 = jnp.float32
BF16 = jnp.bfloat16
VMEM_LIMIT = 60 * 1024 * 1024


def dot(a, b):
    return jnp.dot(a, b, preferred_element_type=F32)


def three_parts(value):
    high = value.astype(BF16)
    rest = value - high.astype(F32)
    mid = rest.astype(BF16)
    low = (rest - mid.astype(F32)).astype(BF16)
    return high, mid, low


def lane_parts(value, heads):
    high, mid, low = three_parts(value)
    group = lax.broadcasted_iota(jnp.int32, value.shape, 1) // heads
    picked = jnp.where(
        group == 0, high.astype(F32), jnp.where(group == 1, mid.astype(F32), low.astype(F32))
    )
    return picked.astype(BF16)


def silu(value):
    half = 0.5 * value
    return half + half * jnp.tanh(half)


def scan_kernel(
    heads,
    remaining,
    tok_ref,
    rim_ref,
    w_ref,
    wstep_ref,
    ck_ref,
    cb_ref,
    sb_ref,
    dr_ref,
    e_ref,
    x_ref,
    bc_ref,
    ec_ref,
    ed_ref,
    cum_ref,
    rt_ref,
    before_ref,
    end_ref,
    raw,
):
    steps = tok_ref.shape[1]
    width = w_ref.shape[1]
    inner = e_ref.shape[1]
    blocks = steps // BLOCK
    taps = ck_ref.shape[0]
    series = pl.program_id(0)
    tokens = tok_ref[0]
    rim = rim_ref[0]

    def convolved(slot, start):
        cols = slice(start, start + CHUNK)
        weights = w_ref[:, cols]
        raw[slot, 0:TAIL, :] = dot(rim, weights).astype(BF16).astype(F32)
        raw[slot, TAIL:, :] = dot(tokens, weights).astype(BF16).astype(F32)
        total = cb_ref[:, cols] + jnp.zeros((steps, CHUNK), F32)
        for tap in range(taps):
            first = TAIL - (taps - 1) + tap
            total = total + ck_ref[tap : tap + 1, cols] * raw[slot, first : first + steps, :]
        return silu(total).astype(BF16)

    bc = convolved(0, inner)
    bc_ref[0] = bc

    step_raw = dot(tokens, wstep_ref[...]) + sb_ref[...]
    soft = jnp.maximum(step_raw, 0.0) + jnp.log1p(jnp.exp(-jnp.abs(step_raw)))
    row = lax.broadcasted_iota(jnp.int32, soft.shape, 0)
    soft = jnp.where(row < remaining[series], soft, 0.0)
    drop = -soft * dr_ref[...]
    below = (
        lax.broadcasted_iota(jnp.int32, (BLOCK, BLOCK), 0)
        >= lax.broadcasted_iota(jnp.int32, (BLOCK, BLOCK), 1)
    ).astype(F32).astype(BF16)
    offset = jnp.zeros((1, LANES), F32)
    weight_parts, decay_rows, b_rows = [], [], []
    for block in range(blocks):
        rows = slice(block * BLOCK, (block + 1) * BLOCK)
        high, mid, low = three_parts(drop[rows])
        cum = dot(below, high) + dot(below, mid) + dot(below, low)
        last = cum[BLOCK - 1 : BLOCK]
        cum_ref[0, rows, :] = cum
        ec_ref[0, rows, :] = lane_parts(jnp.exp(cum), heads)
        ed_ref[0, rows, :] = lane_parts(jnp.exp(cum + offset), heads)
        offset = offset + last
        rt_ref[0, block] = (cum - jnp.log(soft[rows])).T[:heads]
        weight_parts.append(lane_parts(jnp.exp(last - cum) * soft[rows], heads))
        decay_rows.append(lane_parts(jnp.exp(last) + jnp.zeros((TAIL, LANES), F32), heads))
        b_rows.append(bc[rows, :LANES].astype(F32).T.astype(BF16))
    device_row = lane_parts(jnp.exp(offset) + jnp.zeros((TAIL, LANES), F32), heads)

    states = bc.shape[1] // 2
    for index, start in enumerate(range(0, inner, CHUNK)):
        cols = slice(start, start + CHUNK)
        x = convolved((index + 1) % 2, start)
        x_ref[0, :, cols] = x
        state = None
        for block in range(blocks):
            rows = slice(block * BLOCK, (block + 1) * BLOCK)
            wide = dot(weight_parts[block], e_ref[:, cols])
            weighted = (x[rows].astype(F32) * wide).astype(BF16)
            added = dot(b_rows[block], weighted)
            if state is None:
                state = added
            else:
                before_ref[0, block - 1, :, cols] = state.astype(BF16)
                state = dot(decay_rows[block], e_ref[:, cols])[0:1] * state + added
        end_ref[0, 0:states, cols] = state.astype(BF16)
        decay = dot(device_row, e_ref[:, cols])
        high, mid, low = (part.astype(F32) for part in three_parts(decay))
        place = lax.broadcasted_iota(jnp.int32, decay.shape, 0)
        packed = jnp.where(place == 0, high, jnp.where(place == 1, mid, jnp.where(place == 2, low, 0.0)))
        end_ref[0, states:, cols] = packed.astype(BF16)


def within_kernel(heads, x_ref, bc_ref, ec_ref, cum_ref, rt_ref, before_ref, skip_ref, e_ref, out_ref):
    inner = x_ref.shape[2]
    head_size = inner // heads
    here = pl.program_id(1)
    half = BLOCK // 2
    b_part = bc_ref[0, :, :LANES]
    c_part = bc_ref[0, :, LANES:]
    scores = lax.dot_general(c_part, b_part, (((1,), (1,)), ((), ())), preferred_element_type=F32)
    corner = lax.broadcasted_iota(jnp.int32, (half, half), 0) >= lax.broadcasted_iota(
        jnp.int32, (half, half), 1
    )
    earlier = jnp.where(here > 0, c_part.astype(F32), 0.0).astype(BF16)
    cum = cum_ref[0]
    ec = ec_ref[0]
    empty = jnp.zeros((half, half), BF16)
    lane_head = lax.broadcasted_iota(jnp.int32, (BLOCK, CHUNK), 1) // head_size
    for start in range(0, inner, CHUNK):
        cols = slice(start, start + CHUNK)
        x = x_ref[0, :, cols]
        x_wide = x.astype(F32)
        base = skip_ref[:, cols] * x_wide + dot(ec, e_ref[:, cols]) * dot(earlier, before_ref[0, 0, :, cols])
        lefts, rights = [], []
        for local in range(CHUNK // head_size):
            head = start // head_size + local
            at = cum[:, head : head + 1]
            of = rt_ref[0, 0, head : head + 1, :]
            first = jnp.where(corner, jnp.exp(jnp.where(corner, at[:half] - of[:, :half], 0.0)), 0.0)
            middle = jnp.exp(at[half:] - of[:, :half])
            last = jnp.where(corner, jnp.exp(jnp.where(corner, at[half:] - of[:, half:], 0.0)), 0.0)
            top = (first * scores[:half, :half]).astype(BF16)
            left = (middle * scores[half:, :half]).astype(BF16)
            right = (last * scores[half:, half:]).astype(BF16)
            lefts.append(
                jnp.concatenate(
                    [
                        jnp.concatenate([top, empty], axis=1),
                        jnp.concatenate([left, right], axis=1),
                    ],
                    axis=0,
                )
            )
            rights.append(jnp.where(lane_head == local, x_wide, 0.0).astype(BF16))
        mixed = dot(jnp.concatenate(lefts, axis=1), jnp.concatenate(rights, axis=0))
        out_ref[0, :, cols] = (mixed + base).astype(out_ref.dtype)


def out_kernel(
    remaining,
    tok_ref,
    gp_ref,
    part_ref,
    bc_ref,
    ed_ref,
    sin_ref,
    gain_ref,
    op_ref,
    e_ref,
    out_ref,
    gated,
):
    steps = tok_ref.shape[1]
    inner = gp_ref.shape[1]
    series = pl.program_id(0)
    tokens = tok_ref[0]
    c_part = bc_ref[0, :, LANES:]
    ed = ed_ref[0]
    squares = jnp.zeros((steps, LANES), F32)
    for start in range(0, inner, CHUNK):
        cols = slice(start, start + CHUNK)
        gate = dot(tokens, gp_ref[:, cols])
        inter = dot(ed, e_ref[:, cols]) * dot(c_part, sin_ref[0, :, cols])
        value = (part_ref[0, :, cols].astype(F32) + inter) * silu(gate)
        gated[:, cols] = value
        square = value * value
        for lane in range(0, CHUNK, LANES):
            squares = squares + square[:, lane : lane + LANES]
    mean = jnp.sum(squares, axis=1, keepdims=True) / inner
    scale = lax.rsqrt(mean + EPSILON)
    normed = (gated[...] * scale * gain_ref[...]).astype(BF16)
    row = lax.broadcasted_iota(jnp.int32, (steps, CHUNK), 0)
    live = row < remaining[series]
    for start in range(0, op_ref.shape[1], CHUNK):
        cols = slice(start, start + CHUNK)
        result = dot(normed, op_ref[:, cols])
        out_ref[0, :, cols] = jnp.where(live, result, 0.0).astype(BF16)


def whole(shape):
    return pl.BlockSpec(shape, lambda *_: (0,) * len(shape))


def per_series(shape):
    return pl.BlockSpec((1,) + shape, lambda s, *_: (s,) + (0,) * len(shape))


def unpack(packed):
    states = packed.shape[0] - TAIL
    tail = packed[states : states + 3].astype(F32)
    return jnp.sum(tail, axis=0, keepdims=True), packed[:states].astype(F32)


def pack(decay, state):
    high = lax.reduce_precision(decay, 8, 7)
    rest = decay - high
    mid = lax.reduce_precision(rest, 8, 7)
    low = rest - mid
    filler = jnp.zeros((TAIL - 3, decay.shape[1]), F32)
    return jnp.concatenate([state, high, mid, low, filler], axis=0).astype(BF16)


def incoming_state(packed, axis):
    count, mine = lax.axis_size(axis), lax.axis_index(axis)
    half = packed.shape[1] // 2
    odd = mine % 2 == 1
    left, right = packed[:, :half], packed[:, half:]
    swap = [(i, i ^ 1) for i in range(count)]
    own = jnp.where(odd, right, left)
    got = lax.ppermute(jnp.where(odd, left, right), axis, swap)
    first = unpack(jnp.where(odd, got, own))
    second = unpack(jnp.where(odd, own, got))
    total = (first[0] * second[0], second[0] * first[1] + second[1])
    prefix_decay, prefix = jnp.ones_like(first[0]), jnp.zeros_like(first[1])
    bit = 2
    while bit < count:
        final = bit * 2 >= count
        pairs = [(i, i ^ bit) for i in range(count) if not final or not i & bit]
        other = unpack(lax.ppermute(pack(*total), axis, pairs))
        later = (mine & bit) != 0
        prefix = jnp.where(later, prefix_decay * other[1] + prefix, prefix)
        prefix_decay = jnp.where(later, prefix_decay * other[0], prefix_decay)
        if not final:
            total = (
                total[0] * other[0],
                jnp.where(later, total[0] * other[1] + total[1], other[0] * total[1] + other[1]),
            )
        bit *= 2
    behind = (first[0] * prefix + first[1]).astype(BF16)
    prefix = prefix.astype(BF16)
    here = jnp.where(odd, behind, prefix)
    there = lax.ppermute(jnp.where(odd, prefix, behind), axis, swap)
    return jnp.concatenate([jnp.where(odd, there, here), jnp.where(odd, here, there)], axis=1)


def params():
    return pltpu.CompilerParams(vmem_limit_bytes=VMEM_LIMIT)


def body(
    tokens,
    gate_proj,
    input_proj,
    step_proj,
    conv_kernel,
    conv_bias,
    step_bias,
    decay_rate,
    skip_gain,
    norm_gain,
    out_proj,
    lengths,
    slot_series,
):
    series, steps, model = tokens.shape
    inner = gate_proj.shape[1]
    width = input_proj.shape[1]
    states = (width - inner) // 2
    heads = step_bias.shape[0]
    head_size = inner // heads
    blocks = steps // BLOCK
    copies = LANES // heads
    tm, groups = lax.axis_size("tm"), lax.axis_size("series")
    place = lax.axis_index("series")

    taps = conv_kernel.shape[0]
    rim = lax.ppermute(tokens[:, steps - TAIL :], "tm", [(i, i + 1) for i in range(tm - 1)])
    my_lengths = jnp.zeros_like(lengths)
    for shift in range(groups):
        held = lengths
        if shift:
            held = lax.ppermute(lengths, "series", [(i, (i + shift) % groups) for i in range(groups)])
        number = ((place - shift) % groups) * series + jnp.arange(series, dtype=jnp.int32)
        matches = slot_series[:, None] == number[None, :]
        my_lengths = my_lengths + jnp.sum(jnp.where(matches, held[None, :], 0), axis=1)
    remaining = my_lengths - lax.axis_index("tm") * steps

    lane = jnp.arange(LANES)[:, None]
    column = jnp.arange(inner)[None, :]
    expand = ((lane % heads == column // head_size) & (lane < 3 * heads)).astype(BF16)
    step_wide = jnp.tile(step_proj, (1, copies))
    bias_wide = jnp.tile(step_bias, copies)[None]
    rate_wide = jnp.tile(decay_rate, copies)[None]
    skip_wide = jnp.repeat(skip_gain, head_size)[None]

    smem = pl.BlockSpec(memory_space=pltpu.SMEM)
    x, bc, ec, ed, cum, rt, before, end = pl.pallas_call(
        functools.partial(scan_kernel, heads),
        grid=(series,),
        in_specs=[
            smem,
            per_series((steps, model)),
            per_series((TAIL, model)),
            whole((model, width)),
            whole((model, LANES)),
            whole((taps, width)),
            whole((1, width)),
            whole((1, LANES)),
            whole((1, LANES)),
            whole((LANES, inner)),
        ],
        out_specs=[
            per_series((steps, inner)),
            per_series((steps, width - inner)),
            per_series((steps, LANES)),
            per_series((steps, LANES)),
            per_series((steps, LANES)),
            per_series((blocks, heads, BLOCK)),
            per_series((max(blocks - 1, 1), states, inner)),
            per_series((states + TAIL, inner)),
        ],
        out_shape=[
            jax.ShapeDtypeStruct((series, steps, inner), BF16),
            jax.ShapeDtypeStruct((series, steps, width - inner), BF16),
            jax.ShapeDtypeStruct((series, steps, LANES), BF16),
            jax.ShapeDtypeStruct((series, steps, LANES), BF16),
            jax.ShapeDtypeStruct((series, steps, LANES), F32),
            jax.ShapeDtypeStruct((series, blocks, heads, BLOCK), F32),
            jax.ShapeDtypeStruct((series, max(blocks - 1, 1), states, inner), BF16),
            jax.ShapeDtypeStruct((series, states + TAIL, inner), BF16),
        ],
        scratch_shapes=[pltpu.VMEM((2, steps + TAIL, CHUNK), F32)],
        compiler_params=params(),
        cost_estimate=pl.CostEstimate(
            flops=2 * series * steps * model * width, bytes_accessed=16 << 20, transcendentals=0
        ),
        name="scan_terms",
    )(
        remaining,
        tokens,
        rim,
        input_proj,
        step_wide,
        conv_kernel,
        conv_bias[None],
        bias_wide,
        rate_wide,
        expand,
    )

    incoming = jnp.stack([incoming_state(end[s], "tm") for s in range(series)])

    def per_block(shape):
        return pl.BlockSpec((1, BLOCK) + shape, lambda s, b: (s, b) + (0,) * len(shape))

    partial = pl.pallas_call(
        functools.partial(within_kernel, heads),
        grid=(series, blocks),
        in_specs=[
            per_block((inner,)),
            per_block((width - inner,)),
            per_block((LANES,)),
            per_block((LANES,)),
            pl.BlockSpec((1, 1, heads, BLOCK), lambda s, b: (s, b, 0, 0)),
            pl.BlockSpec((1, 1, states, inner), lambda s, b: (s, jnp.maximum(b - 1, 0), 0, 0)),
            whole((1, inner)),
            whole((LANES, inner)),
        ],
        out_specs=per_block((inner,)),
        out_shape=jax.ShapeDtypeStruct((series, steps, inner), BF16),
        compiler_params=params(),
        cost_estimate=pl.CostEstimate(
            flops=16 * series * steps * BLOCK * inner, bytes_accessed=16 << 20, transcendentals=0
        ),
        name="within_blocks",
    )(x, bc, ec, cum, rt, before, skip_wide, expand)

    return pl.pallas_call(
        out_kernel,
        grid=(series,),
        in_specs=[
            smem,
            per_series((steps, model)),
            whole((model, inner)),
            per_series((steps, inner)),
            per_series((steps, width - inner)),
            per_series((steps, LANES)),
            per_series((states, inner)),
            whole((1, inner)),
            whole((inner, model)),
            whole((LANES, inner)),
        ],
        out_specs=per_series((steps, model)),
        out_shape=jax.ShapeDtypeStruct((series, steps, model), BF16),
        scratch_shapes=[pltpu.VMEM((steps, inner), F32)],
        compiler_params=params(),
        cost_estimate=pl.CostEstimate(
            flops=4 * series * steps * model * inner, bytes_accessed=20 << 20, transcendentals=0
        ),
        name="gate_and_out",
    )(remaining, tokens, gate_proj, partial, bc, ed, incoming, norm_gain[None], out_proj, expand)


def solution(mesh):
    in_specs = (P("series", "tm", None),) + (P(),) * 10 + (P("series"), P("series"))
    return jax.shard_map(
        body, mesh=mesh, in_specs=in_specs, out_specs=P("series", "tm", None), check_vma=False
    )
```

```python
import functools

import jax
import jax.numpy as jnp
from jax import lax
from jax.experimental import pallas as pl
from jax.experimental.pallas import tpu as pltpu
from jax.sharding import PartitionSpec as P

BLOCK = 256
CHUNK = 256
LANES = 128
TAIL = 16
ROWS = 64
EPSILON = 1e-05
F32 = jnp.float32
BF16 = jnp.bfloat16
VMEM_LIMIT = 60 * 1024 * 1024


def dot(a, b):
    return jnp.dot(a, b, preferred_element_type=F32)


def three_parts(value):
    high = value.astype(BF16)
    rest = value - high.astype(F32)
    mid = rest.astype(BF16)
    low = (rest - mid.astype(F32)).astype(BF16)
    return high, mid, low


def lane_parts(value, heads):
    high, mid, low = three_parts(value)
    group = lax.broadcasted_iota(jnp.int32, value.shape, 1) // heads
    picked = jnp.where(
        group == 0, high.astype(F32), jnp.where(group == 1, mid.astype(F32), low.astype(F32))
    )
    return picked.astype(BF16)


def expand_columns(heads, head_size, start):
    lane = lax.broadcasted_iota(jnp.int32, (LANES, CHUNK), 0)
    column = start + lax.broadcasted_iota(jnp.int32, (LANES, CHUNK), 1)
    same = (lane % heads == column // head_size) & (lane < 3 * heads)
    return jnp.where(same, 1.0, 0.0).astype(BF16)


def head_row(heads, ref):
    lane = lax.broadcasted_iota(jnp.int32, (1, LANES), 1) % heads
    row = jnp.zeros((1, LANES), F32)
    for head in range(heads):
        row = jnp.where(lane == head, ref[head], row)
    return row


def steps_left(held_refs, slot_ref, series, steps):
    groups = len(held_refs)
    place = lax.axis_index("series")
    slot = slot_ref[series]
    total = jnp.int32(0)
    for shift, ref in enumerate(held_refs):
        first = lax.rem(place - shift + groups, groups) * ref.shape[0]
        for index in range(ref.shape[0]):
            total = total + jnp.where(slot == first + index, ref[index], 0)
    return total - lax.axis_index("tm") * steps


def silu(value):
    half = 0.5 * value
    return half + half * jnp.tanh(half)


def scan_kernel(heads, groups, *refs):
    held_refs, refs = refs[:groups], refs[groups:]
    (slot_ref, sb_ref, dr_ref, tok_ref, rim_ref, w_ref, wstep_ref, ck_ref, cb_ref), refs = (
        refs[:9],
        refs[9:],
    )
    x_ref, bc_ref, ec_ref, ed_ref, cum_ref, rt_ref, before_ref, end_ref, raw = refs
    steps = tok_ref.shape[1]
    inner = x_ref.shape[2]
    head_size = inner // heads
    blocks = steps // BLOCK
    taps = ck_ref.shape[0]
    series = pl.program_id(0)
    tokens = tok_ref[0]
    rim = rim_ref[0]

    def convolved(slot, start, put):
        cols = slice(start, start + CHUNK)
        weights = w_ref[:, cols]
        raw[slot, 0:TAIL, :] = dot(rim, weights).astype(BF16).astype(F32)
        raw[slot, TAIL:, :] = dot(tokens, weights).astype(BF16).astype(F32)
        bias = cb_ref[cols][None, :]
        gains = [ck_ref[tap : tap + 1, cols] for tap in range(taps)]
        for row in range(0, steps, ROWS):
            total = bias
            for tap in range(taps):
                first = TAIL - (taps - 1) + tap + row
                total = total + gains[tap] * raw[slot, first : first + ROWS, :]
            put(slice(row, row + ROWS), silu(total).astype(BF16))

    def put_bc(rows, value):
        bc_ref[0, rows, :] = value

    convolved(0, inner, put_bc)
    bc = bc_ref[0]

    wstep = jnp.concatenate([wstep_ref[...]] * (LANES // heads), axis=0)
    step_raw = lax.dot_general(
        tokens, wstep, (((1,), (1,)), ((), ())), preferred_element_type=F32
    ) + head_row(heads, sb_ref)
    soft = jnp.maximum(step_raw, 0.0) + jnp.log1p(jnp.exp(-jnp.abs(step_raw)))
    row = lax.broadcasted_iota(jnp.int32, soft.shape, 0)
    soft = jnp.where(row < steps_left(held_refs, slot_ref, series, steps), soft, 0.0)
    drop = -soft * head_row(heads, dr_ref)
    below = (
        lax.broadcasted_iota(jnp.int32, (BLOCK, BLOCK), 0)
        >= lax.broadcasted_iota(jnp.int32, (BLOCK, BLOCK), 1)
    ).astype(F32).astype(BF16)
    offset = jnp.zeros((1, LANES), F32)
    weight_parts, decay_rows, b_rows = [], [], []
    for block in range(blocks):
        rows = slice(block * BLOCK, (block + 1) * BLOCK)
        high, mid, low = three_parts(drop[rows])
        cum = dot(below, high) + dot(below, mid) + dot(below, low)
        last = cum[BLOCK - 1 : BLOCK]
        cum_ref[0, rows, :] = cum
        ec_ref[0, rows, :] = lane_parts(jnp.exp(cum), heads)
        ed_ref[0, rows, :] = lane_parts(jnp.exp(cum + offset), heads)
        offset = offset + last
        rt_ref[0, block] = (cum - jnp.log(soft[rows])).T[:heads]
        weight_parts.append(lane_parts(jnp.exp(last - cum) * soft[rows], heads))
        decay_rows.append(lane_parts(jnp.exp(last) + jnp.zeros((TAIL, LANES), F32), heads))
        b_rows.append(bc[rows, :LANES].astype(F32).T.astype(BF16))
    device_row = lane_parts(jnp.exp(offset) + jnp.zeros((TAIL, LANES), F32), heads)

    states = bc.shape[1] // 2
    for index, start in enumerate(range(0, inner, CHUNK)):
        cols = slice(start, start + CHUNK)

        def put_x(rows, value, cols=cols):
            x_ref[0, rows, cols] = value

        convolved((index + 1) % 2, start, put_x)
        spread = expand_columns(heads, head_size, start)
        state = None
        for block in range(blocks):
            rows = slice(block * BLOCK, (block + 1) * BLOCK)
            wide = dot(weight_parts[block], spread)
            weighted = (x_ref[0, rows, cols].astype(F32) * wide).astype(BF16)
            added = dot(b_rows[block], weighted)
            if state is None:
                state = added
            else:
                before_ref[0, block - 1, :, cols] = state.astype(BF16)
                state = dot(decay_rows[block], spread)[0:1] * state + added
        end_ref[0, 0:states, cols] = state.astype(BF16)
        decay = dot(device_row, spread)
        high, mid, low = (part.astype(F32) for part in three_parts(decay))
        place = lax.broadcasted_iota(jnp.int32, decay.shape, 0)
        packed = jnp.where(place == 0, high, jnp.where(place == 1, mid, jnp.where(place == 2, low, 0.0)))
        end_ref[0, states:, cols] = packed.astype(BF16)


def within_kernel(heads, skip_ref, x_ref, bc_ref, ec_ref, cum_ref, rt_ref, before_ref, *rest):
    out_ref = rest[-1]
    inner = x_ref.shape[2]
    head_size = inner // heads
    here = pl.program_id(0)
    half = BLOCK // 2
    b_part = bc_ref[0, :, :LANES]
    c_part = bc_ref[0, :, LANES:]
    scores = lax.dot_general(c_part, b_part, (((1,), (1,)), ((), ())), preferred_element_type=F32)
    corner = lax.broadcasted_iota(jnp.int32, (half, half), 0) >= lax.broadcasted_iota(
        jnp.int32, (half, half), 1
    )
    earlier = jnp.where(here > 0, c_part.astype(F32), 0.0).astype(BF16)
    cum = cum_ref[0]
    ec = ec_ref[0]
    empty = jnp.zeros((half, half), BF16)
    lane_head = lax.broadcasted_iota(jnp.int32, (BLOCK, CHUNK), 1) // head_size
    for start in range(0, inner, CHUNK):
        cols = slice(start, start + CHUNK)
        x = x_ref[0, :, cols]
        x_wide = x.astype(F32)
        skip = jnp.zeros((1, CHUNK), F32)
        for local in range(CHUNK // head_size):
            skip = jnp.where(lane_head[:1] == local, skip_ref[start // head_size + local], skip)
        wide = dot(ec, expand_columns(heads, head_size, start))
        base = skip * x_wide + wide * dot(earlier, before_ref[0, 0, :, cols])
        lefts, rights = [], []
        for local in range(CHUNK // head_size):
            head = start // head_size + local
            at = cum[:, head : head + 1]
            of = rt_ref[0, 0, head : head + 1, :]
            first = jnp.where(corner, jnp.exp(jnp.where(corner, at[:half] - of[:, :half], 0.0)), 0.0)
            middle = jnp.exp(at[half:] - of[:, :half])
            last = jnp.where(corner, jnp.exp(jnp.where(corner, at[half:] - of[:, half:], 0.0)), 0.0)
            top = (first * scores[:half, :half]).astype(BF16)
            left = (middle * scores[half:, :half]).astype(BF16)
            right = (last * scores[half:, half:]).astype(BF16)
            lefts.append(
                jnp.concatenate(
                    [
                        jnp.concatenate([top, empty], axis=1),
                        jnp.concatenate([left, right], axis=1),
                    ],
                    axis=0,
                )
            )
            rights.append(jnp.where(lane_head == local, x_wide, 0.0).astype(BF16))
        mixed = dot(jnp.concatenate(lefts, axis=1), jnp.concatenate(rights, axis=0))
        out_ref[0, :, cols] = (mixed + base).astype(out_ref.dtype)


def gate_kernel(tok_ref, gp_ref, out_ref):
    tokens = tok_ref[0]
    for start in range(0, gp_ref.shape[1], CHUNK):
        cols = slice(start, start + CHUNK)
        out_ref[0, :, cols] = silu(dot(tokens, gp_ref[:, cols])).astype(BF16)


def out_kernel(heads, groups, count, *refs):
    held_refs, slot_ref, refs = refs[:groups], refs[groups], refs[groups + 1 :]
    gate_ref, part_ref, bc_ref, ed_ref, gain_ref, op_ref = refs[:6]
    sin_refs, out_ref, gated = refs[6 : 6 + count], refs[-2], refs[-1]
    steps = gate_ref.shape[1]
    inner = gate_ref.shape[2]
    head_size = inner // heads
    series = pl.program_id(0)
    c_part = bc_ref[0, :, LANES:]
    ed = ed_ref[0]
    squares = jnp.zeros((steps, LANES), F32)
    for start in range(0, inner, CHUNK):
        cols = slice(start, start + CHUNK)
        state = sin_refs[0][:, cols]
        for index in range(1, count):
            state = jnp.where(series == index, sin_refs[index][:, cols], state)
        inter = dot(ed, expand_columns(heads, head_size, start)) * dot(c_part, state)
        value = (part_ref[0, :, cols].astype(F32) + inter) * gate_ref[0, :, cols].astype(F32)
        gated[:, cols] = value
        square = value * value
        for lane in range(0, CHUNK, LANES):
            squares = squares + square[:, lane : lane + LANES]
    mean = jnp.sum(squares, axis=1, keepdims=True) / inner
    scale = lax.rsqrt(mean + EPSILON)
    normed = jnp.concatenate(
        [
            (gated[:, start : start + CHUNK] * scale * gain_ref[start : start + CHUNK][None, :]).astype(BF16)
            for start in range(0, inner, CHUNK)
        ],
        axis=1,
    )
    row = lax.broadcasted_iota(jnp.int32, (steps, CHUNK), 0)
    live = row < steps_left(held_refs, slot_ref, series, steps)
    for start in range(0, op_ref.shape[1], CHUNK):
        cols = slice(start, start + CHUNK)
        result = dot(normed, op_ref[:, cols])
        out_ref[0, :, cols] = jnp.where(live, result, 0.0).astype(BF16)


def whole(shape):
    return pl.BlockSpec(shape, lambda *_: (0,) * len(shape))


def per_series(shape):
    return pl.BlockSpec((1,) + shape, lambda s, *_: (s,) + (0,) * len(shape))


def unpack(packed):
    states = packed.shape[0] - TAIL
    tail = packed[states : states + 3].astype(F32)
    return jnp.sum(tail, axis=0, keepdims=True), packed[:states].astype(F32)


def pack(decay, state):
    high = lax.reduce_precision(decay, 8, 7)
    rest = decay - high
    mid = lax.reduce_precision(rest, 8, 7)
    low = rest - mid
    filler = jnp.zeros((TAIL - 3, decay.shape[1]), F32)
    return jnp.concatenate([state, high, mid, low, filler], axis=0).astype(BF16)


def incoming_states(packed, axis, covers):
    count, mine = lax.axis_size(axis), lax.axis_index(axis)
    lanes = range(len(packed))
    half = packed[0].shape[1] // 2
    odd = mine % 2 == 1
    swap = [(i, i ^ 1) for i in range(count)]
    firsts, totals, prefixes = [], [], []
    for one in packed:
        left, right = one[:, :half], one[:, half:]
        got = lax.ppermute(jnp.where(odd, left, right), axis, swap)
        own = jnp.where(odd, right, left)
        first = unpack(jnp.where(odd, got, own))
        second = unpack(jnp.where(odd, own, got))
        firsts.append(first)
        totals.append((first[0] * second[0], second[0] * first[1] + second[1]))
        prefixes.append((jnp.ones_like(first[0]), jnp.zeros_like(first[1])))
    bit = 2
    while bit < count:
        final = bit * 2 >= count
        pairs = [(i, i ^ bit) for i in range(count) if not final or not i & bit]
        later = (mine & bit) != 0
        for lane in lanes:
            total, prefix = totals[lane], prefixes[lane]
            sent = pack(*total)
            if covers and (bit > 2 or lane == lanes[-1]):
                sent = covers.pop(0)(sent)
            other = unpack(lax.ppermute(sent, axis, pairs))
            prefixes[lane] = (
                jnp.where(later, prefix[0] * other[0], prefix[0]),
                jnp.where(later, prefix[0] * other[1] + prefix[1], prefix[1]),
            )
            if not final:
                totals[lane] = (
                    total[0] * other[0],
                    jnp.where(later, total[0] * other[1] + total[1], other[0] * total[1] + other[1]),
                )
        bit *= 2
    outs = []
    for lane in lanes:
        first, prefix = firsts[lane], prefixes[lane][1]
        behind = (first[0] * prefix + first[1]).astype(BF16)
        prefix = prefix.astype(BF16)
        here = jnp.where(odd, behind, prefix)
        there = lax.ppermute(jnp.where(odd, prefix, behind), axis, swap)
        outs.append(
            jnp.concatenate([jnp.where(odd, there, here), jnp.where(odd, here, there)], axis=1)
        )
    return outs


def params():
    return pltpu.CompilerParams(vmem_limit_bytes=VMEM_LIMIT)


def body(
    tokens,
    gate_proj,
    input_proj,
    step_proj,
    conv_kernel,
    conv_bias,
    step_bias,
    decay_rate,
    skip_gain,
    norm_gain,
    out_proj,
    lengths,
    slot_series,
):
    series, steps, model = tokens.shape
    inner = gate_proj.shape[1]
    width = input_proj.shape[1]
    states = (width - inner) // 2
    heads = step_bias.shape[0]
    blocks = steps // BLOCK
    tm, groups = lax.axis_size("tm"), lax.axis_size("series")
    taps = conv_kernel.shape[0]
    rim = lax.ppermute(tokens[:, steps - TAIL :], "tm", [(i, i + 1) for i in range(tm - 1)])
    held = [lengths]
    for shift in range(1, groups):
        held.append(lax.ppermute(lengths, "series", [(i, (i + shift) % groups) for i in range(groups)]))

    smem = pl.BlockSpec(memory_space=pltpu.SMEM)
    x, bc, ec, ed, cum, rt, before, end = pl.pallas_call(
        functools.partial(scan_kernel, heads, groups),
        grid=(series,),
        in_specs=[
            *[smem] * (groups + 3),
            per_series((steps, model)),
            per_series((TAIL, model)),
            whole((model, width)),
            whole((heads, model)),
            whole((taps, width)),
            whole((width,)),
        ],
        out_specs=[
            per_series((steps, inner)),
            per_series((steps, width - inner)),
            per_series((steps, LANES)),
            per_series((steps, LANES)),
            per_series((steps, LANES)),
            per_series((blocks, heads, BLOCK)),
            per_series((max(blocks - 1, 1), states, inner)),
            per_series((states + TAIL, inner)),
        ],
        out_shape=[
            jax.ShapeDtypeStruct((series, steps, inner), BF16),
            jax.ShapeDtypeStruct((series, steps, width - inner), BF16),
            jax.ShapeDtypeStruct((series, steps, LANES), BF16),
            jax.ShapeDtypeStruct((series, steps, LANES), BF16),
            jax.ShapeDtypeStruct((series, steps, LANES), F32),
            jax.ShapeDtypeStruct((series, blocks, heads, BLOCK), F32),
            jax.ShapeDtypeStruct((series, max(blocks - 1, 1), states, inner), BF16),
            jax.ShapeDtypeStruct((series, states + TAIL, inner), BF16),
        ],
        scratch_shapes=[pltpu.VMEM((2, steps + TAIL, CHUNK), F32)],
        compiler_params=params(),
        cost_estimate=pl.CostEstimate(
            flops=2 * series * steps * model * width, bytes_accessed=16 << 20, transcendentals=0
        ),
        name="scan_terms",
    )(
        *held,
        slot_series,
        step_bias,
        decay_rate,
        tokens,
        rim,
        input_proj,
        step_proj.T,
        conv_kernel,
        conv_bias,
    )

    def within(one, cum, partial):
        def per_block(shape):
            return pl.BlockSpec((1, BLOCK) + shape, lambda b: (one, b) + (0,) * len(shape))

        earlier = [] if partial is None else [partial]
        return pl.pallas_call(
            functools.partial(within_kernel, heads),
            grid=(blocks,),
            in_specs=[
                smem,
                per_block((inner,)),
                per_block((width - inner,)),
                per_block((LANES,)),
                per_block((LANES,)),
                pl.BlockSpec((1, 1, heads, BLOCK), lambda b: (one, b, 0, 0)),
                pl.BlockSpec((1, 1, states, inner), lambda b: (one, jnp.maximum(b - 1, 0), 0, 0)),
            ]
            + [pl.BlockSpec(memory_space=pl.ANY)] * len(earlier),
            out_specs=per_block((inner,)),
            out_shape=jax.ShapeDtypeStruct((series, steps, inner), BF16),
            input_output_aliases={7: 0} if earlier else {},
            compiler_params=params(),
            cost_estimate=pl.CostEstimate(
                flops=16 * steps * BLOCK * inner, bytes_accessed=8 << 20, transcendentals=0
            ),
            name="within_blocks",
        )(skip_gain, x, bc, ec, cum, rt, before, *earlier)

    done = {"cum": cum, "partial": None}

    def cover_within(one):
        def run(sent):
            sent, ready = lax.optimization_barrier((sent, done["cum"]))
            done["partial"] = within(one, ready, done["partial"])
            return sent

        return run

    def gates(tokens):
        return pl.pallas_call(
            gate_kernel,
            grid=(series,),
            in_specs=[per_series((steps, model)), whole((model, inner))],
            out_specs=per_series((steps, inner)),
            out_shape=jax.ShapeDtypeStruct((series, steps, inner), BF16),
            compiler_params=params(),
            cost_estimate=pl.CostEstimate(
                flops=2 * series * steps * model * inner, bytes_accessed=10 << 20, transcendentals=0
            ),
            name="gates",
        )(tokens, gate_proj)

    def cover_gates(sent):
        sent, ready = lax.optimization_barrier((sent, tokens))
        done["gate"] = gates(ready)
        return sent

    covers = [cover_within(one) for one in range(series)] + [cover_gates]
    incoming = incoming_states([end[s] for s in range(series)], "tm", covers)
    for cover in covers:
        cover(incoming[-1])

    return pl.pallas_call(
        functools.partial(out_kernel, heads, groups, series),
        grid=(series,),
        in_specs=[
            *[smem] * (groups + 1),
            per_series((steps, inner)),
            per_series((steps, inner)),
            per_series((steps, width - inner)),
            per_series((steps, LANES)),
            whole((inner,)),
            whole((inner, model)),
        ]
        + [whole((states, inner))] * series,
        out_specs=per_series((steps, model)),
        out_shape=jax.ShapeDtypeStruct((series, steps, model), BF16),
        scratch_shapes=[pltpu.VMEM((steps, inner), F32)],
        compiler_params=params(),
        cost_estimate=pl.CostEstimate(
            flops=2 * series * steps * model * inner, bytes_accessed=16 << 20, transcendentals=0
        ),
        name="gate_and_out",
    )(*held, slot_series, done["gate"], done["partial"], bc, ed, norm_gain, out_proj, *incoming)


def solution(mesh):
    in_specs = (P("series", "tm", None),) + (P(),) * 10 + (P("series"), P("series"))
    return jax.shard_map(
        body, mesh=mesh, in_specs=in_specs, out_specs=P("series", "tm", None), check_vma=False
    )
```
